32 devices in a mesh: fsdp: 16 (over z, y, x), model: 2 (over core).
Axes of the slice: x: 2, y: 2, z: 4, core: 2. Of those that a mesh axis runs over, the one named last changes fastest.
Arguments:
- train_query: float32 [2560, 4096], P('fsdp', 'model'), may hold values from -0.15625 to 0.15625
- drift_query: float32 [2560, 4096], P('fsdp', 'model'), may hold values from -6 to 6
- spread_query: float32 [2560, 4096], P('fsdp', 'model'), may hold values from 0.1 to 10
- train_key: float32 [2560, 1024], P('fsdp', 'model'), may hold values from -0.15625 to 0.15625
- drift_key: float32 [2560, 1024], P('fsdp', 'model'), may hold values from -6 to 6
- spread_key: float32 [2560, 1024], P('fsdp', 'model'), may hold values from 0.1 to 10
- train_value: float32 [2560, 1024], P('fsdp', 'model'), may hold values from -0.15625 to 0.15625
- drift_value: float32 [2560, 1024], P('fsdp', 'model'), may hold values from -6 to 6
- spread_value: float32 [2560, 1024], P('fsdp', 'model'), may hold values from 0.1 to 10
- norm_train: float32 [2560], P(('fsdp', 'model')), may hold values from 0.25 to 1.75
- norm_step: float32 [2560], P(('fsdp', 'model')), may hold values from -0.3 to 0.3
Outputs:
- serve_query: bfloat16 [2560, 4096], P(None, 'model')
- serve_key: bfloat16 [2560, 1024], P(None, 'model')
- serve_value: bfloat16 [2560, 1024], P(None, 'model')
- factor_query: float32 [4096], P('model')
- factor_key: float32 [1024], P('model')
- factor_value: float32 [1024], P('model')
- serve_norm: bfloat16 [2560], replicated
- fresh_query: float32 [2560, 4096], P('fsdp', 'model')
- fresh_key: float32 [2560, 1024], P('fsdp', 'model')
- fresh_value: float32 [2560, 1024], P('fsdp', 'model')
The draws below stay inside these ranges and needn't reach their ends.
All inputs are finite; a program needn't handle non-finite values. Where the reference program divides by a largest or mean magnitude, that divisor is 1e-20 or more.
Results may differ from the reference program's by a relative error of at most 0.001.
Values may be sent and summed in bfloat16 or wider, within the bound.
A program may use at most 64 MiB of HBM per device.

```python
import math
import jax
import jax.numpy as jnp
from jax import lax

D_MODEL = 2560
Q_DIM = 4096
KV_DIM = 1024


def raised(result, rng, source, target, parts, factor):
    owner, partner = [(jnp.arange(result.shape[dim]) // (result.shape[dim] // parts)).reshape([-1 if axis == dim else 1 for axis in range(result.ndim)]) for dim in (source, target)]
    chosen = jax.random.permutation(rng, parts)[partner]
    strong = (owner == chosen) | (owner == (partner + parts // 2) % parts)
    return jnp.where(strong, factor * result, result)


def block_scale(rng, dims, pieces, low, high):
    factor_of = 1.0
    for axis_at, shards_of in pieces:
        draws = jax.random.uniform(jax.random.fold_in(jax.random.fold_in(rng, 6), axis_at), (shards_of,), jnp.float32, low / len(pieces), high / len(pieces))
        factor_of = factor_of * jnp.repeat(jnp.exp(draws), dims[axis_at] // shards_of).reshape((-1,) + (1,) * (len(dims) - 1 - axis_at))
    return factor_of


def scatter_about(stream_key, extent, spread, bound, shards=(), dtype=jnp.bfloat16):
    drawn = jax.random.normal(stream_key, extent, jnp.float32) * spread
    if len(shards) > 0:
        drawn = block_scale(stream_key, extent, shards, -0.22, 0.18) * drawn
    return jnp.clip(drawn, min=-bound, max=bound).astype(dtype)


def gaussian_with(own_key, extent, deviation, limit, split, heavy, kind=jnp.bfloat16):
    entries = deviation * jax.random.normal(own_key, extent, jnp.float32)
    if split:
        entries = entries * block_scale(own_key, extent, split, -0.22, 0.18)
    return jnp.clip(raised(entries, jax.random.fold_in(own_key, 3), *heavy), -limit, limit).astype(kind)


def setup_inputs(seed: int = 0) -> dict:
    arg_keys = jax.random.split(jax.random.key(seed), 12)
    train_query = gaussian_with(arg_keys[0], (D_MODEL, Q_DIM), D_MODEL ** -0.5, 0.15625, ((0, 16), (1, 2)), (0, 1, 16, 2.0), jnp.float32)
    drift_query = scatter_about(arg_keys[1], (D_MODEL, Q_DIM), 1.0, 6.0, ((0, 16), (1, 2)), jnp.float32)
    spread_query = jnp.clip(jnp.exp(math.log(10.0) - 4.6051702 * jax.random.uniform(arg_keys[2], (D_MODEL, Q_DIM), jnp.float32) ** block_scale(arg_keys[2], (D_MODEL, Q_DIM), ((0, 16), (1, 2)), -0.2, 0.2)), 0.1, 10.0)
    train_key = gaussian_with(arg_keys[3], (D_MODEL, KV_DIM), D_MODEL ** -0.5, 0.15625, ((0, 16), (1, 2)), (0, 1, 16, 2.0), jnp.float32)
    drift_key = scatter_about(arg_keys[4], (D_MODEL, KV_DIM), 1.0, 6.0, ((0, 16), (1, 2)), jnp.float32)
    spread_key = jnp.clip(jnp.exp(math.log(10.0) - 4.6051702 * jax.random.uniform(arg_keys[5], (D_MODEL, KV_DIM), jnp.float32) ** block_scale(arg_keys[5], (D_MODEL, KV_DIM), ((0, 16), (1, 2)), -0.2, 0.2)), 0.1, 10.0)
    train_value = gaussian_with(arg_keys[6], (D_MODEL, KV_DIM), D_MODEL ** -0.5, 0.15625, ((0, 16), (1, 2)), (0, 1, 16, 2.0), jnp.float32)
    drift_value = scatter_about(arg_keys[7], (D_MODEL, KV_DIM), 1.0, 6.0, ((0, 16), (1, 2)), jnp.float32)
    spread_value = jnp.clip(jnp.exp(math.log(10.0) - 4.6051702 * jax.random.uniform(arg_keys[8], (D_MODEL, KV_DIM), jnp.float32) ** block_scale(arg_keys[8], (D_MODEL, KV_DIM), ((0, 16), (1, 2)), -0.2, 0.2)), 0.1, 10.0)
    norm_train = jnp.clip(1.0 + 0.15 * jax.random.normal(arg_keys[9], (D_MODEL,), jnp.float32), 0.25, 1.75)
    norm_step = jnp.clip(jax.random.uniform(arg_keys[10], (D_MODEL,), jnp.float32, -0.3, 0.3) * block_scale(arg_keys[10], (D_MODEL,), ((0, 32),), -0.4, 0.0), -0.3, 0.3)
    return dict(train_query=train_query, drift_query=drift_query, spread_query=spread_query, train_key=train_key, drift_key=drift_key, spread_key=spread_key, train_value=train_value, drift_value=drift_value, spread_value=spread_value, norm_train=norm_train, norm_step=norm_step)


learn_rate = 0.02
decay_rate = 0.05
tiny_value = 1e-08

def reference(train_query, drift_query, spread_query, train_key, drift_key, spread_key, train_value, drift_value, spread_value, norm_train, norm_step):
    fresh_query = train_query - learn_rate * (drift_query / (jnp.sqrt(spread_query) + tiny_value) + decay_rate * train_query)
    fresh_key = train_key - learn_rate * (drift_key / (jnp.sqrt(spread_key) + tiny_value) + decay_rate * train_key)
    fresh_value = train_value - learn_rate * (drift_value / (jnp.sqrt(spread_value) + tiny_value) + decay_rate * train_value)
    factor_query = lax.optimization_barrier(jnp.max(jnp.abs(fresh_query), axis=0))
    serve_query = (fresh_query / factor_query).astype(jnp.bfloat16)
    factor_key = lax.optimization_barrier(jnp.max(jnp.abs(fresh_key), axis=0))
    serve_key = (fresh_key / factor_key).astype(jnp.bfloat16)
    factor_value = lax.optimization_barrier(jnp.max(jnp.abs(fresh_value), axis=0))
    serve_value = (fresh_value / factor_value).astype(jnp.bfloat16)
    serve_norm = (norm_train + norm_step).astype(jnp.bfloat16)
    return (serve_query, serve_key, serve_value, factor_query, factor_key, factor_value, serve_norm, fresh_query, fresh_key, fresh_value)
```

```python
import functools

import jax
import jax.numpy as jnp
from jax import lax
from jax.experimental import pallas as pl
from jax.experimental.pallas import tpu as pltpu
from jax.sharding import PartitionSpec as P

learn_rate = 0.02
decay_rate = 0.05
tiny_value = 1e-08
MESH = pl.DeviceIdType.MESH
ROWS = 16
LANES = 128

AZ, BZ, AX, AXF, AY, AYF, BX, BXF, BY, BYF, COUNT = 0, 4, 20, 24, 28, 32, 36, 37, 38, 39, 40


def stepped(train, drift, spread):
    return train - learn_rate * (drift / (jnp.sqrt(spread) + tiny_value) + decay_rate * train)


def gather_kernel(
    part_a, fresh_q, fresh_k, fresh_v, norm_row, held, factor, norms,
    mx, mx_send, mx_recv, nm_send, nm_recv, send, recv,
):
    f = lax.axis_index("fsdp")
    m = lax.axis_index("model")
    z = f // 4
    r = f % 4
    y = r // 2
    x = r % 2
    rx, ry, rd = y * 2 + (1 - x), (1 - y) * 2 + x, (1 - y) * 2 + (1 - x)
    rows = fresh_q.shape[0]
    widths = (fresh_q.shape[1], fresh_k.shape[1], fresh_v.shape[1])
    starts = (0, widths[0], widths[0] + widths[1])
    fresh = (fresh_q, fresh_k, fresh_v)
    half_a = part_a // 2
    half_b = (rows - part_a) // 2

    def device(zz, rr):
        return {"fsdp": zz * 4 + rr, "model": m}

    plane = [device(z, rx), device(z, ry), device(z, rd)]
    line = [device((z + k) % 4, r) for k in range(1, 4)]
    partner = {"fsdp": f, "model": 1 - m}

    barrier = pltpu.get_barrier_semaphore()
    for peer in plane + line + [partner]:
        pl.semaphore_signal(barrier, inc=1, device_id=peer, device_id_type=MESH)

    for ref, start, width in zip(fresh, starts, widths):
        step = min(512, width)
        for c in range(0, width, step):
            def body(i, acc, ref=ref, c=c, step=step):
                return jnp.maximum(acc, jnp.abs(ref[pl.ds(i * 8, 8), c : c + step]))
            acc = lax.fori_loop(0, rows // 8, body, jnp.zeros((8, step), jnp.float32), unroll=4)
            mx[0, :, start + c : start + c + step] = jnp.max(acc, axis=0, keepdims=True)
    norms[m, f] = norm_row[...]

    pl.semaphore_wait(barrier, 7)

    def remote(src, dst, s, d, peer):
        return pltpu.make_async_remote_copy(
            src_ref=src, dst_ref=dst, send_sem=s, recv_sem=d, device_id=peer, device_id_type=MESH
        )

    small = []
    for k, peer in enumerate(plane):
        copy = remote(mx.at[0], mx.at[1 + k], mx_send.at[k], mx_recv.at[k], peer)
        copy.start()
        small.append(copy)
    tags = []
    for k, peer in enumerate(plane):
        copy = remote(norms.at[m, f], norms.at[m, f], nm_send.at[k], nm_recv.at[k], peer)
        copy.start()
        tags.append(copy)
    for copy in small:
        copy.wait_recv()
    mx[4] = jnp.maximum(jnp.maximum(mx[0], mx[1]), jnp.maximum(mx[2], mx[3]))
    for k, peer in enumerate(line):
        copy = remote(mx.at[4], mx.at[5 + k], mx_send.at[3 + k], mx_recv.at[3 + k], peer)
        copy.start()
        small.append(copy)
    for k, rr in enumerate((rx, ry, rd)):
        mine = norms.at[m, z * 4 + rr]
        remote(mine, mine, nm_send.at[k], nm_recv.at[k], plane[k]).wait_recv()
    group = norms.at[m, pl.ds(z * 4, 4)]
    for k, peer in enumerate(line):
        copy = remote(group, group, nm_send.at[3 + k], nm_recv.at[3 + k], peer)
        copy.start()
        tags.append(copy)
    for copy in small[3:]:
        copy.wait_recv()
    factor[...] = jnp.maximum(jnp.maximum(mx[4], mx[5]), jnp.maximum(mx[6], mx[7]))

    def narrow(first, last):
        def body(i, carry):
            at = pl.ds(pl.multiple_of(first + i * ROWS, ROWS), ROWS)
            for ref, start, width in zip(fresh, starts, widths):
                step = min(512, width)
                for c in range(0, width, step):
                    scale = factor[:, start + c : start + c + step]
                    held[f, at, start + c : start + c + step] = (
                        ref[at, c : c + step] / scale
                    ).astype(jnp.bfloat16)
            return carry
        lax.fori_loop(0, (last - first) // ROWS, body, 0)

    done = []

    def piece(zz, rr, first, last):
        return held.at[zz * 4 + rr, pl.ds(first, last - first)]

    def copy_of(zz, rr, first, last, s, d, peer):
        block = piece(zz, rr, first, last)
        return remote(block, block, send.at[s], recv.at[d], peer)

    def go(make):
        make().start()
        done.append(make)

    def got(zz, rr, first, last, d):
        copy_of(zz, rr, first, last, d, d, plane[0]).wait_recv()

    hi = z // 2
    z_end, z_mid, z_mid2, z_end2 = 3 * hi, 1 + hi, 2 - hi, 3 - 3 * hi
    is_end = z == z_end
    is_mid = z == z_mid
    near = z_end + z_mid - z
    plane_of = (r, rx, ry, rd)

    def az(zz, to, outward):
        go(lambda: copy_of(zz, r, 0, part_a, AZ + zz + (COUNT if outward else 0), AZ + zz, device(to, r)))

    def bz(zz, j, to, outward):
        def make():
            at = BZ + zz * 4 + j
            back = at + (COUNT if outward else 0)
            return copy_of(zz, plane_of[j], part_a, rows, back, at, device(to, r))
        go(make)

    def got_az(zz):
        got(zz, r, 0, part_a, AZ + zz)

    def got_bz(zz, j):
        got(zz, plane_of[j], part_a, rows, BZ + zz * 4 + j)

    def a_own(zz):
        go(lambda: copy_of(zz, r, 0, part_a, AX + zz, AX + zz, plane[0]))
        go(lambda: copy_of(zz, r, 0, part_a, AY + zz, AY + zz, plane[1]))

    def a_forward(zz):
        got(zz, rx, 0, part_a, AX + zz)
        go(lambda: copy_of(zz, rx, half_a, part_a, AYF + zz, AYF + zz, plane[1]))
        got(zz, ry, 0, part_a, AY + zz)
        go(lambda: copy_of(zz, ry, 0, half_a, AXF + zz, AXF + zz, plane[0]))

    narrow(part_a, rows)
    go(lambda: copy_of(z, r, part_a, rows, BX, BX, plane[0]))
    go(lambda: copy_of(z, r, part_a, rows, BY, BY, plane[1]))
    narrow(0, part_a)

    tail = []

    def branch(pred):
        def wrap(body):
            @pl.when(pred)
            def _():
                kept = list(done)
                done.clear()
                body()
                tail.append((pred, list(done)))
                done.clear()
                done.extend(kept)
        return wrap

    @branch(is_end)
    def _():
        az(z_end, z_mid, False)

    @branch(is_mid)
    def _():
        az(z_mid, z_mid2, False)
        az(z_mid, z_end, True)

    a_own(z)
    got(z, rx, part_a, rows, BX)
    go(lambda: copy_of(z, rx, part_a + half_b, rows, BYF, BYF, plane[1]))
    got(z, ry, part_a, rows, BY)
    go(lambda: copy_of(z, ry, part_a, part_a + half_b, BXF, BXF, plane[0]))

    @branch(is_end)
    def _():
        for j in (0, 1):
            bz(z_end, j, z_mid, False)
        got_az(z_mid)

    @branch(is_mid)
    def _():
        for j in (0, 1):
            bz(z_mid, j, z_mid2, False)
            bz(z_mid, j, z_end, True)
        got_az(z_end)
        az(z_end, z_mid2, False)
        got_az(z_mid2)
        az(z_mid2, z_end, True)

    a_own(near)
    got(z, rd, part_a, part_a + half_b, BXF)
    got(z, rd, part_a + half_b, rows, BYF)

    @branch(is_end)
    def _():
        for j in (2, 3):
            bz(z_end, j, z_mid, False)

    @branch(is_mid)
    def _():
        for j in (2, 3):
            bz(z_mid, j, z_mid2, False)
            bz(z_mid, j, z_end, True)

    a_forward(z)

    @branch(is_end)
    def _():
        got_az(z_mid2)

    a_own(z_mid2)

    @branch(is_mid)
    def _():
        got_az(z_end2)
        az(z_end2, z_end, True)

    a_forward(near)

    @branch(is_mid)
    def _():
        for j in range(4):
            got_bz(z_end, j)
            bz(z_end, j, z_mid2, False)
        for j in range(4):
            got_bz(z_mid2, j)
            bz(z_mid2, j, z_end, True)

    @branch(is_end)
    def _():
        got_az(z_end2)

    a_own(z_end2)
    a_forward(z_mid2)

    @branch(is_mid)
    def _():
        for j in range(4):
            got_bz(z_end2, j)
            bz(z_end2, j, z_end, True)

    for k in range(1, 4):
        theirs = norms.at[m, pl.ds(((z + 4 - k) % 4) * 4, 4)]
        remote(theirs, theirs, nm_send.at[2 + k], nm_recv.at[2 + k], line[k - 1]).wait_recv()
    whole = norms.at[m]
    copy = remote(whole, whole, nm_send.at[6], nm_recv.at[6], partner)
    copy.start()
    tags.append(copy)

    a_forward(z_end2)

    @branch(is_end)
    def _():
        for zz in (z_mid, z_mid2, z_end2):
            for j in range(4):
                got_bz(zz, j)

    for zz in (z, near, z_mid2, z_end2):
        got(zz, rd, 0, half_a, AXF + zz)
        got(zz, rd, half_a, part_a, AYF + zz)
    theirs = norms.at[1 - m]
    remote(theirs, theirs, nm_send.at[6], nm_recv.at[6], partner).wait_recv()
    for copy in small + tags:
        copy.wait_send()
    for make in done:
        make().wait_send()
    for pred in (is_end, is_mid):
        @pl.when(pred)
        def _(pred=pred):
            for which, copies in tail:
                if which is pred:
                    for make in copies:
                        make().wait_send()


def with_kernel(part_a, *args):
    (tq, dq, sq, tk, dk, sk, tv, dv, sv, norm_train, norm_step) = args
    fq, fk, fv = stepped(tq, dq, sq), stepped(tk, dk, sk), stepped(tv, dv, sv)
    norm = norm_train + norm_step
    length = norm.shape[0]
    padded = -(-length // LANES) * LANES
    norm_row = jnp.pad(norm, (0, padded - length)).reshape(1, padded)
    n, cores = lax.axis_size("fsdp"), lax.axis_size("model")
    rows = tq.shape[0]
    wq, wk, wv = tq.shape[1], tk.shape[1], tv.shape[1]
    width = wq + wk + wv
    vmem = pl.BlockSpec(memory_space=pltpu.VMEM)
    held, factor, norms = pl.pallas_call(
        functools.partial(gather_kernel, part_a),
        out_shape=(
            pltpu.VMEM((n, rows, width), jnp.bfloat16),
            jax.ShapeDtypeStruct((1, width), jnp.float32),
            jax.ShapeDtypeStruct((cores, n, 1, padded), jnp.float32),
        ),
        in_specs=[vmem] * 4,
        out_specs=(vmem, vmem, vmem),
        scratch_shapes=[
            pltpu.VMEM((8, 1, width), jnp.float32),
            pltpu.SemaphoreType.DMA((6,)),
            pltpu.SemaphoreType.DMA((6,)),
            pltpu.SemaphoreType.DMA((7,)),
            pltpu.SemaphoreType.DMA((7,)),
            pltpu.SemaphoreType.DMA((COUNT + AX,)),
            pltpu.SemaphoreType.DMA((COUNT,)),
        ],
        compiler_params=pltpu.CompilerParams(
            collective_id=0, has_side_effects=True, vmem_limit_bytes=24 * 1024 * 1024
        ),
    )(fq, fk, fv, norm_row)
    served = held.reshape(n * rows, width)
    factor = factor.reshape(width)
    serve_norm = (
        norms[:, :, 0, :length].transpose(1, 0, 2).reshape(n * cores * length).astype(jnp.bfloat16)
    )
    return (
        served[:, :wq], served[:, wq : wq + wk], served[:, wq + wk :],
        factor[:wq], factor[wq : wq + wk], factor[wq + wk :],
        serve_norm, fq, fk, fv,
    )


def per_device(
    train_query,
    drift_query,
    spread_query,
    train_key,
    drift_key,
    spread_key,
    train_value,
    drift_value,
    spread_value,
    norm_train,
    norm_step,
):
    n, cores, rows = lax.axis_size("fsdp"), lax.axis_size("model"), train_query.shape[0]
    part_a = rows - (rows * 2 // 9 // (2 * ROWS)) * 2 * ROWS
    lanes_ok = all(a.shape[1] % LANES == 0 for a in (train_query, train_key, train_value))
    if n == 16 and cores == 2 and rows % (2 * ROWS) == 0 and part_a < rows and lanes_ok:
        return with_kernel(
            part_a,
            train_query, drift_query, spread_query,
            train_key, drift_key, spread_key,
            train_value, drift_value, spread_value,
            norm_train, norm_step,
        )
    fresh_query = train_query - learn_rate * (
        drift_query / (jnp.sqrt(spread_query) + tiny_value) + decay_rate * train_query
    )
    fresh_key = train_key - learn_rate * (
        drift_key / (jnp.sqrt(spread_key) + tiny_value) + decay_rate * train_key
    )
    fresh_value = train_value - learn_rate * (
        drift_value / (jnp.sqrt(spread_value) + tiny_value) + decay_rate * train_value
    )
    factor_query, factor_key, factor_value = lax.pmax(
        (
            jnp.max(jnp.abs(fresh_query), axis=0),
            jnp.max(jnp.abs(fresh_key), axis=0),
            jnp.max(jnp.abs(fresh_value), axis=0),
        ),
        "fsdp",
    )
    narrow_query, narrow_key, narrow_value = (
        (fresh_query / factor_query).astype(jnp.bfloat16),
        (fresh_key / factor_key).astype(jnp.bfloat16),
        (fresh_value / factor_value).astype(jnp.bfloat16),
    )
    serve_query, serve_key, serve_value = (
        lax.all_gather(narrow_query, "fsdp", axis=0, tiled=True),
        lax.all_gather(narrow_key, "fsdp", axis=0, tiled=True),
        lax.all_gather(narrow_value, "fsdp", axis=0, tiled=True),
    )
    serve_norm = lax.all_gather(
        (norm_train + norm_step).astype(jnp.bfloat16), ("fsdp", "model"), axis=0, tiled=True
    )
    return (
        serve_query,
        serve_key,
        serve_value,
        factor_query,
        factor_key,
        factor_value,
        serve_norm,
        fresh_query,
        fresh_key,
        fresh_value,
    )


def solution(mesh):
    in_specs = (
        P("fsdp", "model"),
        P("fsdp", "model"),
        P("fsdp", "model"),
        P("fsdp", "model"),
        P("fsdp", "model"),
        P("fsdp", "model"),
        P("fsdp", "model"),
        P("fsdp", "model"),
        P("fsdp", "model"),
        P(("fsdp", "model")),
        P(("fsdp", "model")),
    )
    out_specs = (
        P(None, "model"),
        P(None, "model"),
        P(None, "model"),
        P("model"),
        P("model"),
        P("model"),
        P(),
        P("fsdp", "model"),
        P("fsdp", "model"),
        P("fsdp", "model"),
    )
    return jax.shard_map(
        per_device, mesh=mesh, in_specs=in_specs, out_specs=out_specs, check_vma=False
    )
```

```python
import functools

import jax
import jax.numpy as jnp
from jax import lax
from jax.experimental import pallas as pl
from jax.experimental.pallas import tpu as pltpu
from jax.sharding import PartitionSpec as P

learn_rate = 0.02
decay_rate = 0.05
tiny_value = 1e-08
MESH = pl.DeviceIdType.MESH
ROWS = 16
CHUNK = 32
VMEM_BYTES = 67043328
LANES = 128

AZ, BZ, AX, AXF, AY, AYF, BXF, BYF, COUNT = 0, 4, 20, 24, 28, 32, 36, 37, 38


def stepped(train, drift, spread):
    return train - learn_rate * (drift / (jnp.sqrt(spread) + tiny_value) + decay_rate * train)


def gather_kernel(
    part_a,
    tq, dq, sq, tk, dk, sk, tv, dv, sv, norm_train, norm_step,
    held, fresh_q, fresh_k, fresh_v, factor, norms,
    in_q, in_k, in_v, norm_in, top, early_q, early_k, early_v,
    mx, in_sem, norm_sem, mx_send, mx_recv, nm_send, nm_recv, early_send, early_recv, send, recv,
):
    f = lax.axis_index("fsdp")
    m = lax.axis_index("model")
    z = f // 4
    r = f % 4
    y = r // 2
    x = r % 2
    rx, ry, rd = y * 2 + (1 - x), (1 - y) * 2 + x, (1 - y) * 2 + (1 - x)
    rows = fresh_q.shape[0]
    widths = (fresh_q.shape[1], fresh_k.shape[1], fresh_v.shape[1])
    starts = (0, widths[0], widths[0] + widths[1])
    fresh = (fresh_q, fresh_k, fresh_v)
    early = (early_q, early_k, early_v)
    inputs = ((tq, dq, sq), (tk, dk, sk), (tv, dv, sv))
    local = (in_q, in_k, in_v)
    half_a = part_a // 2
    half_b = (rows - part_a) // 2

    def device(zz, rr):
        return {"fsdp": zz * 4 + rr, "model": m}

    plane = [device(z, rx), device(z, ry), device(z, rd)]
    line = [device((z + k) % 4, r) for k in range(1, 4)]
    partner = {"fsdp": f, "model": 1 - m}

    barrier = pltpu.get_barrier_semaphore()
    for peer in plane + line + [partner]:
        pl.semaphore_signal(barrier, inc=1, device_id=peer, device_id_type=MESH)

    def loads(i):
        at = pl.ds(pl.multiple_of(i * CHUNK, CHUNK), CHUNK)
        return [
            pltpu.make_async_copy(src.at[at], local[a].at[k, at], in_sem.at[i, a * 3 + k])
            for a in range(3)
            for k, src in enumerate(inputs[a])
        ]

    for i in range(rows // CHUNK):
        for copy in loads(i):
            copy.start()
    norm_loads = [
        pltpu.make_async_copy(src, norm_in.at[k], norm_sem.at[k])
        for k, src in enumerate((norm_train, norm_step))
    ]
    for copy in norm_loads:
        copy.start()

    top[...] = jnp.zeros_like(top)

    def chunk(i, carry):
        copies = loads(i)
        for a, (ref, start, width) in enumerate(zip(fresh, starts, widths)):
            for copy in copies[a * 3 : a * 3 + 3]:
                copy.wait()
            step = min(512, width)
            for c in range(0, width, step):
                cols = slice(c, c + step)
                best = top[:, start + c : start + c + step]
                for g in range(CHUNK // 8):
                    at = pl.ds(pl.multiple_of(i * CHUNK + g * 8, 8), 8)
                    new = stepped(local[a][0, at, cols], local[a][1, at, cols], local[a][2, at, cols])
                    ref[at, cols] = new
                    best = jnp.maximum(best, jnp.abs(new))
                top[:, start + c : start + c + step] = best
        return carry

    lax.fori_loop(0, rows // CHUNK, chunk, 0)
    mx[0] = jnp.max(top[...], axis=0, keepdims=True)
    for copy in norm_loads:
        copy.wait()
    norms[m, f] = jnp.zeros_like(norms[m, f])
    norms[m, f, :, : norm_in.shape[2]] = norm_in[0] + norm_in[1]

    pl.semaphore_wait(barrier, 7)

    def remote(src, dst, s, d, peer):
        return pltpu.make_async_remote_copy(
            src_ref=src, dst_ref=dst, send_sem=s, recv_sem=d, device_id=peer, device_id_type=MESH
        )

    small = []
    for k, peer in enumerate(plane):
        copy = remote(mx.at[0], mx.at[1 + k], mx_send.at[k], mx_recv.at[k], peer)
        copy.start()
        small.append(copy)
    tags = []
    for k, peer in enumerate(plane):
        copy = remote(norms.at[m, f], norms.at[m, f], nm_send.at[k], nm_recv.at[k], peer)
        copy.start()
        tags.append(copy)
    ahead = []
    for k in range(2):
        for a in range(3):
            copy = remote(
                fresh[a].at[pl.ds(part_a, rows - part_a)], early[a].at[k],
                early_send.at[k * 3 + a], early_recv.at[k * 3 + a], plane[k],
            )
            copy.start()
            ahead.append(copy)
    for copy in small:
        copy.wait_recv()
    mx[4] = jnp.maximum(jnp.maximum(mx[0], mx[1]), jnp.maximum(mx[2], mx[3]))
    for k, peer in enumerate(line):
        copy = remote(mx.at[4], mx.at[5 + k], mx_send.at[3 + k], mx_recv.at[3 + k], peer)
        copy.start()
        small.append(copy)
    for k, rr in enumerate((rx, ry, rd)):
        mine = norms.at[m, z * 4 + rr]
        remote(mine, mine, nm_send.at[k], nm_recv.at[k], plane[k]).wait_recv()
    group = norms.at[m, pl.ds(z * 4, 4)]
    for k, peer in enumerate(line):
        copy = remote(group, group, nm_send.at[3 + k], nm_recv.at[3 + k], peer)
        copy.start()
        tags.append(copy)
    for copy in small[3:]:
        copy.wait_recv()
    factor[...] = jnp.maximum(jnp.maximum(mx[4], mx[5]), jnp.maximum(mx[6], mx[7]))

    def narrow(refs, skip, block, first, last):
        def body(i, carry):
            at = pl.ds(pl.multiple_of(first + i * ROWS, ROWS), ROWS)
            here = pl.ds(pl.multiple_of(first - skip + i * ROWS, ROWS), ROWS)
            for ref, start, width in zip(refs, starts, widths):
                step = min(512, width)
                for c in range(0, width, step):
                    scale = factor[:, start + c : start + c + step]
                    held[block, at, start + c : start + c + step] = (
                        ref[here, c : c + step] / scale
                    ).astype(jnp.bfloat16)
            return carry
        lax.fori_loop(0, (last - first) // ROWS, body, 0)

    done = []

    def piece(zz, rr, first, last):
        return held.at[zz * 4 + rr, pl.ds(first, last - first)]

    def copy_of(zz, rr, first, last, s, d, peer):
        block = piece(zz, rr, first, last)
        return remote(block, block, send.at[s], recv.at[d], peer)

    def go(make):
        make().start()
        done.append(make)

    def got(zz, rr, first, last, d):
        copy_of(zz, rr, first, last, d, d, plane[0]).wait_recv()

    hi = z // 2
    z_end, z_mid, z_mid2, z_end2 = 3 * hi, 1 + hi, 2 - hi, 3 - 3 * hi
    is_end = z == z_end
    is_mid = z == z_mid
    near = z_end + z_mid - z
    plane_of = (r, rx, ry, rd)

    def az(zz, to, outward):
        go(lambda: copy_of(zz, r, 0, part_a, AZ + zz + (COUNT if outward else 0), AZ + zz, device(to, r)))

    def bz(zz, j, to, outward):
        def make():
            at = BZ + zz * 4 + j
            back = at + (COUNT if outward else 0)
            return copy_of(zz, plane_of[j], part_a, rows, back, at, device(to, r))
        go(make)

    def got_az(zz):
        got(zz, r, 0, part_a, AZ + zz)

    def got_bz(zz, j):
        got(zz, plane_of[j], part_a, rows, BZ + zz * 4 + j)

    def a_own(zz):
        go(lambda: copy_of(zz, r, 0, part_a, AX + zz, AX + zz, plane[0]))
        go(lambda: copy_of(zz, r, 0, part_a, AY + zz, AY + zz, plane[1]))

    def a_forward(zz):
        got(zz, rx, 0, part_a, AX + zz)
        go(lambda: copy_of(zz, rx, half_a, part_a, AYF + zz, AYF + zz, plane[1]))
        got(zz, ry, 0, part_a, AY + zz)
        go(lambda: copy_of(zz, ry, 0, half_a, AXF + zz, AXF + zz, plane[0]))

    narrow(fresh, 0, f, 0, part_a)

    tail = []

    def branch(pred):
        def wrap(body):
            @pl.when(pred)
            def _():
                kept = list(done)
                done.clear()
                body()
                tail.append((pred, list(done)))
                done.clear()
                done.extend(kept)
        return wrap

    @branch(is_end)
    def _():
        az(z_end, z_mid, False)

    @branch(is_mid)
    def _():
        az(z_mid, z_mid2, False)
        az(z_mid, z_end, True)

    a_own(z)
    narrow(fresh, 0, f, part_a, rows)
    for k, rr in enumerate((rx, ry)):
        for copy in ahead[k * 3 : k * 3 + 3]:
            copy.wait_recv()
        narrow([ref.at[k] for ref in early], part_a, z * 4 + rr, part_a, rows)
        if k == 0:
            go(lambda: copy_of(z, rx, part_a + half_b, rows, BYF, BYF, plane[1]))
    go(lambda: copy_of(z, ry, part_a, part_a + half_b, BXF, BXF, plane[0]))

    @branch(is_end)
    def _():
        for j in (0, 1):
            bz(z_end, j, z_mid, False)
        got_az(z_mid)

    @branch(is_mid)
    def _():
        for j in (0, 1):
            bz(z_mid, j, z_mid2, False)
            bz(z_mid, j, z_end, True)
        got_az(z_end)
        az(z_end, z_mid2, False)
        got_az(z_mid2)
        az(z_mid2, z_end, True)

    a_own(near)
    got(z, rd, part_a, part_a + half_b, BXF)
    got(z, rd, part_a + half_b, rows, BYF)

    @branch(is_end)
    def _():
        for j in (2, 3):
            bz(z_end, j, z_mid, False)

    @branch(is_mid)
    def _():
        for j in (2, 3):
            bz(z_mid, j, z_mid2, False)
            bz(z_mid, j, z_end, True)

    a_forward(z)

    @branch(is_end)
    def _():
        got_az(z_mid2)

    a_own(z_mid2)

    @branch(is_mid)
    def _():
        got_az(z_end2)
        az(z_end2, z_end, True)

    a_forward(near)

    @branch(is_mid)
    def _():
        for j in range(4):
            got_bz(z_end, j)
            bz(z_end, j, z_mid2, False)
        for j in range(4):
            got_bz(z_mid2, j)
            bz(z_mid2, j, z_end, True)

    @branch(is_end)
    def _():
        got_az(z_end2)

    a_own(z_end2)
    a_forward(z_mid2)

    @branch(is_mid)
    def _():
        for j in range(4):
            got_bz(z_end2, j)
            bz(z_end2, j, z_end, True)

    for k in range(1, 4):
        theirs = norms.at[m, pl.ds(((z + 4 - k) % 4) * 4, 4)]
        remote(theirs, theirs, nm_send.at[2 + k], nm_recv.at[2 + k], line[k - 1]).wait_recv()
    whole = norms.at[m]
    copy = remote(whole, whole, nm_send.at[6], nm_recv.at[6], partner)
    copy.start()
    tags.append(copy)

    a_forward(z_end2)

    @branch(is_end)
    def _():
        for zz in (z_mid, z_mid2, z_end2):
            for j in range(4):
                got_bz(zz, j)

    for zz in (z, near, z_mid2, z_end2):
        got(zz, rd, 0, half_a, AXF + zz)
        got(zz, rd, half_a, part_a, AYF + zz)
    theirs = norms.at[1 - m]
    remote(theirs, theirs, nm_send.at[6], nm_recv.at[6], partner).wait_recv()
    for copy in small + tags + ahead:
        copy.wait_send()
    for make in done:
        make().wait_send()
    for pred in (is_end, is_mid):
        @pl.when(pred)
        def _(pred=pred):
            for which, copies in tail:
                if which is pred:
                    for make in copies:
                        make().wait_send()


def write_kernel(held, fresh_q, fresh_k, fresh_v, factor, *rest):
    serve, rates, fresh_out, sems = rest[:3], rest[3:6], rest[6:9], rest[9]
    n = held.shape[0]
    cut = max(1, n // 4)
    copies = []
    start = 0
    for k in range(3):
        width = serve[k].shape[2]
        for b in range(0, n, cut):
            copies.append((held.at[pl.ds(b, cut), :, pl.ds(start, width)], serve[k].at[pl.ds(b, cut)]))
        copies.append((factor.at[:, pl.ds(start, width)], rates[k]))
        copies.append(((fresh_q, fresh_k, fresh_v)[k], fresh_out[k]))
        start += width
    copies = [pltpu.make_async_copy(src, dst, sems.at[i]) for i, (src, dst) in enumerate(copies)]
    for copy in copies:
        copy.start()
    for copy in copies:
        copy.wait()


def with_kernel(part_a, *args):
    (tq, dq, sq, tk, dk, sk, tv, dv, sv, norm_train, norm_step) = args
    length = norm_train.shape[0]
    padded = -(-length // LANES) * LANES
    n, cores = lax.axis_size("fsdp"), lax.axis_size("model")
    rows = tq.shape[0]
    widths = (tq.shape[1], tk.shape[1], tv.shape[1])
    width = sum(widths)
    vmem = pl.BlockSpec(memory_space=pltpu.VMEM)
    hbm = pl.BlockSpec(memory_space=pltpu.HBM)
    f32, bf16 = jnp.float32, jnp.bfloat16
    room = VMEM_BYTES - n * rows * width * 2 - rows * width * 4 - 192 * 1024
    held, fresh_q, fresh_k, fresh_v, factor, norms = pl.pallas_call(
        functools.partial(gather_kernel, part_a),
        out_shape=(
            pltpu.VMEM((n, rows, width), bf16),
            *[pltpu.VMEM((rows, w), f32) for w in widths],
            pltpu.VMEM((1, width), f32),
            jax.ShapeDtypeStruct((cores, n, 1, padded), f32),
        ),
        in_specs=[hbm] * 11,
        out_specs=(vmem,) * 6,
        scratch_shapes=[
            *[pltpu.VMEM((3, rows, w), f32) for w in widths],
            pltpu.VMEM((2, 1, length), f32),
            pltpu.VMEM((8, width), f32),
            *[pltpu.VMEM((2, rows - part_a, w), f32) for w in widths],
            pltpu.VMEM((8, 1, width), f32),
            pltpu.SemaphoreType.DMA((rows // CHUNK, 9)),
            pltpu.SemaphoreType.DMA((2,)),
            pltpu.SemaphoreType.DMA((6,)),
            pltpu.SemaphoreType.DMA((6,)),
            pltpu.SemaphoreType.DMA((7,)),
            pltpu.SemaphoreType.DMA((7,)),
            pltpu.SemaphoreType.DMA((6,)),
            pltpu.SemaphoreType.DMA((6,)),
            pltpu.SemaphoreType.DMA((COUNT + AX,)),
            pltpu.SemaphoreType.DMA((COUNT,)),
        ],
        compiler_params=pltpu.CompilerParams(
            collective_id=0, has_side_effects=True, vmem_limit_bytes=room
        ),
        name="gather",
    )(
        tq, dq, sq, tk, dk, sk, tv, dv, sv,
        norm_train.reshape(1, length), norm_step.reshape(1, length),
    )
    out = pl.pallas_call(
        write_kernel,
        out_shape=(
            *[jax.ShapeDtypeStruct((n, rows, w), bf16) for w in widths],
            *[jax.ShapeDtypeStruct((1, w), f32) for w in widths],
            *[jax.ShapeDtypeStruct((rows, w), f32) for w in widths],
        ),
        in_specs=[vmem] * 5,
        out_specs=(hbm,) * 9,
        scratch_shapes=[pltpu.SemaphoreType.DMA((18,))],
        compiler_params=pltpu.CompilerParams(vmem_limit_bytes=4 * 1024 * 1024),
        name="write",
    )(held, fresh_q, fresh_k, fresh_v, factor)
    serve_norm = (
        norms[:, :, 0, :length].transpose(1, 0, 2).reshape(n * cores * length).astype(bf16)
    )
    return (
        *[a.reshape(n * rows, w) for a, w in zip(out[:3], widths)],
        *[a.reshape(w) for a, w in zip(out[3:6], widths)],
        serve_norm, *out[6:],
    )


def per_device(
    train_query,
    drift_query,
    spread_query,
    train_key,
    drift_key,
    spread_key,
    train_value,
    drift_value,
    spread_value,
    norm_train,
    norm_step,
):
    n, cores, rows = lax.axis_size("fsdp"), lax.axis_size("model"), train_query.shape[0]
    part_a = rows - (rows * 2 // 9 // (2 * ROWS)) * 2 * ROWS
    lanes_ok = all(a.shape[1] % LANES == 0 for a in (train_query, train_key, train_value))
    if n == 16 and cores == 2 and rows % CHUNK == 0 and part_a < rows and lanes_ok:
        return with_kernel(
            part_a,
            train_query, drift_query, spread_query,
            train_key, drift_key, spread_key,
            train_value, drift_value, spread_value,
            norm_train, norm_step,
        )
    fresh_query = train_query - learn_rate * (
        drift_query / (jnp.sqrt(spread_query) + tiny_value) + decay_rate * train_query
    )
    fresh_key = train_key - learn_rate * (
        drift_key / (jnp.sqrt(spread_key) + tiny_value) + decay_rate * train_key
    )
    fresh_value = train_value - learn_rate * (
        drift_value / (jnp.sqrt(spread_value) + tiny_value) + decay_rate * train_value
    )
    factor_query, factor_key, factor_value = lax.pmax(
        (
            jnp.max(jnp.abs(fresh_query), axis=0),
            jnp.max(jnp.abs(fresh_key), axis=0),
            jnp.max(jnp.abs(fresh_value), axis=0),
        ),
        "fsdp",
    )
    narrow_query, narrow_key, narrow_value = (
        (fresh_query / factor_query).astype(jnp.bfloat16),
        (fresh_key / factor_key).astype(jnp.bfloat16),
        (fresh_value / factor_value).astype(jnp.bfloat16),
    )
    serve_query, serve_key, serve_value = (
        lax.all_gather(narrow_query, "fsdp", axis=0, tiled=True),
        lax.all_gather(narrow_key, "fsdp", axis=0, tiled=True),
        lax.all_gather(narrow_value, "fsdp", axis=0, tiled=True),
    )
    serve_norm = lax.all_gather(
        (norm_train + norm_step).astype(jnp.bfloat16), ("fsdp", "model"), axis=0, tiled=True
    )
    return (
        serve_query,
        serve_key,
        serve_value,
        factor_query,
        factor_key,
        factor_value,
        serve_norm,
        fresh_query,
        fresh_key,
        fresh_value,
    )


def solution(mesh):
    in_specs = (
        P("fsdp", "model"),
        P("fsdp", "model"),
        P("fsdp", "model"),
        P("fsdp", "model"),
        P("fsdp", "model"),
        P("fsdp", "model"),
        P("fsdp", "model"),
        P("fsdp", "model"),
        P("fsdp", "model"),
        P(("fsdp", "model")),
        P(("fsdp", "model")),
    )
    out_specs = (
        P(None, "model"),
        P(None, "model"),
        P(None, "model"),
        P("model"),
        P("model"),
        P("model"),
        P(),
        P("fsdp", "model"),
        P("fsdp", "model"),
        P("fsdp", "model"),
    )
    return jax.shard_map(
        per_device, mesh=mesh, in_specs=in_specs, out_specs=out_specs, check_vma=False
    )
```
